32 devices in a mesh: feat: 16 (over z, y, x), samp: 2 (over core).
Axes of the slice: x: 2, y: 2, z: 4, core: 2. Of those that a mesh axis runs over, the one named last changes fastest.
Arguments:
- features: bfloat16 [256, 131072], P('samp', 'feat'), may hold values from -14 to 14
- labels: int32 [256, 32], P('samp'), may hold values from -1 to 1, as said below
- alpha_start: float32 [256, 32], P('samp'), may hold values from 0 to 1
- order: int32 [2, 256], P(None, 'samp'), may hold values from 0 to 127, as said below
Outputs:
- alpha: float32 [256, 32], P('samp')
- scores: float32 [256, 32], P('samp')
The draws below stay inside these ranges and needn't reach their ends.
Inputs may be any that keep to these rules, and one draw needn't show every extreme that they name: `labels`: every entry is -1 or +1. `order`: for each round, each aligned block of 128 entries (one partition) is a permutation of 0 to 127.
All inputs are finite; a program needn't handle non-finite values.
Results may differ from the reference program's by a relative error of at most 0.004.
Values may be sent and summed in bfloat16 or wider, within the bound.
A program may use at most 64 MiB of HBM per device.

```python
import math
import jax
import jax.numpy as jnp
from jax import lax

FEAT_DEV = 8192
LABELS = 32
ROWS_DEV = 128
BLOCK = 64
ROUNDS = 2
FEATURES = 131072
ROWS = 256


def draw_features(key, part):
    key_values, key_scale, key_common, key_coef = jax.random.split(jax.random.fold_in(key, 11), 4)
    group_width = FEAT_DEV // 2
    group_count = FEATURES // group_width
    log_scale = jax.random.uniform(key_scale, (group_count,), jnp.float32, math.log(0.35), math.log(2.8))
    column_scale = jnp.repeat(jnp.exp(log_scale), group_width)
    raw_values = jnp.clip(jax.random.normal(key_values, (ROWS, FEATURES), jnp.float32), -5.0, 5.0)
    return (raw_values * column_scale[None, :]).astype(jnp.bfloat16)


def draw_labels(key, part):
    coins = jax.random.randint(jax.random.fold_in(key, 23), (ROWS, LABELS), 0, 2, dtype=jnp.int32)
    return (2 * coins - 1).astype(jnp.int32)


def draw_order(key, part):
    part_total = ROWS // ROWS_DEV
    subkeys = jax.random.split(jax.random.fold_in(key, 37), ROUNDS * part_total)
    perms = jax.vmap(lambda subkey: jax.random.permutation(subkey, ROWS_DEV))(subkeys)
    return perms.reshape(ROUNDS, ROWS).astype(jnp.int32)


def levels(own_key, shape, cuts, low, high):
    loudness, own = 1.0, jax.random.fold_in(own_key, 6)
    for dim, blocks in cuts:
        heights = jnp.exp(jax.random.uniform(jax.random.fold_in(own, dim), (blocks,), jnp.float32, low / len(cuts), high / len(cuts)))
        loudness = loudness * jnp.repeat(heights, shape[dim] // blocks).reshape([-1 if axis == dim else 1 for axis in range(len(shape))])
    return loudness


def setup_inputs(seed: int = 0) -> dict:
    streams_of = jax.random.split(jax.random.key(seed), 5)
    features = draw_features(jax.random.fold_in(streams_of[4], 71), 0)
    labels = draw_labels(jax.random.fold_in(streams_of[4], 71), 0)
    alpha_start = jnp.clip(1.0 * jax.random.uniform(streams_of[2], (ROWS, LABELS), jnp.float32) ** levels(streams_of[2], (ROWS, LABELS), ((0, 2),), -0.2, 0.2), 0.0, 1.0)
    order = draw_order(jax.random.fold_in(streams_of[4], 71), 0)
    return dict(features=features, labels=labels, alpha_start=alpha_start, order=order)


reg_scale = 0.9


def part_slice(source, part_index):
    return lax.dynamic_slice_in_dim(source, part_index * ROWS_DEV, ROWS_DEV, 0)


def contract_rows(left_side, right_side):
    return lax.dot_general(left_side, right_side, (((0,), (0,)), ((), ())), preferred_element_type=jnp.float32)


def contract_cols(left_side, right_side):
    return lax.dot_general(left_side, right_side, (((1,), (1,)), ((), ())), preferred_element_type=jnp.float32)


def local_round(weights, part_rows, part_signs, part_alpha, part_norms, row_order, lam_total):
    local_weights = weights
    local_alpha = part_alpha
    for block_num in range(ROWS_DEV // BLOCK):
        chosen = row_order[block_num * BLOCK:(block_num + 1) * BLOCK]
        picked = jnp.take(part_rows, chosen, axis=0)
        margins = contract_cols(picked, local_weights.astype(jnp.bfloat16))
        before = jnp.take(local_alpha, chosen, axis=0)
        block_signs = jnp.take(part_signs, chosen, axis=0)
        block_norms = jnp.take(part_norms, chosen, axis=0)
        updated = jnp.clip(before + lam_total * (1.0 - block_signs * margins) / block_norms[:, None], 0.0, 1.0)
        change = ((updated - before) * block_signs).astype(jnp.bfloat16)
        local_alpha = local_alpha.at[chosen].set(updated)
        local_weights = local_weights + contract_rows(change, picked) / lam_total
    return local_weights, local_alpha


def reference(features, labels, alpha_start, order):
    part_count = ROWS // ROWS_DEV
    lam_total = reg_scale * FEATURES
    signs_all = labels.astype(jnp.float32)
    part_ids = jnp.arange(part_count, dtype=jnp.int32)

    def row_norms(part_index):
        part_rows = part_slice(features, part_index)
        return jnp.einsum("rf,rf->r", part_rows, part_rows, preferred_element_type=jnp.float32) + 1.0

    norms_all = lax.map(row_norms, part_ids)

    def warm_part(running, part_index):
        part_rows = part_slice(features, part_index)
        coeffs = (part_slice(alpha_start, part_index) * part_slice(signs_all, part_index)).astype(jnp.bfloat16)
        piece = lax.optimization_barrier((contract_rows(coeffs, part_rows) / lam_total).astype(jnp.bfloat16))
        return running + piece.astype(jnp.float32), None

    weights, _ = lax.scan(warm_part, jnp.zeros((LABELS, FEATURES), jnp.float32), part_ids)
    alpha_now = alpha_start
    for round_num in range(ROUNDS):
        def round_part(running, part_index, weights=weights, alpha_now=alpha_now, round_num=round_num):
            part_alpha = part_slice(alpha_now, part_index)
            row_order = lax.dynamic_slice_in_dim(order[round_num], part_index * ROWS_DEV, ROWS_DEV, 0)
            local_weights, local_alpha = local_round(weights, part_slice(features, part_index), part_slice(signs_all, part_index), part_alpha, norms_all[part_index], row_order, lam_total)
            delta_weights = lax.optimization_barrier((local_weights - weights).astype(jnp.bfloat16))
            return running + delta_weights.astype(jnp.float32), part_alpha + (local_alpha - part_alpha) / part_count

        summed, alpha_parts = lax.scan(round_part, jnp.zeros((LABELS, FEATURES), jnp.float32), part_ids)
        weights = weights + summed / part_count
        alpha_now = alpha_parts.reshape(ROWS, LABELS)
    weights_half = weights.astype(jnp.bfloat16)

    def score_part(part_index):
        return contract_cols(part_slice(features, part_index), weights_half)

    scores = lax.map(score_part, part_ids).reshape(ROWS, LABELS)
    return alpha_now, scores
```

```python
import functools

import jax
import jax.numpy as jnp
from jax import lax
from jax.experimental import pallas as pl
from jax.experimental.pallas import tpu as pltpu
from jax.sharding import PartitionSpec as P

BLOCK = 64
ROUNDS = 2
REG_SCALE = 0.9
PIECES = 2


def round_up(value, unit):
    return (value + unit - 1) // unit * unit


def gram_of(left, right):
    return lax.dot_general(
        left, right, (((1,), (1,)), ((), ())), preferred_element_type=jnp.float32
    )


def wrap(value, size):
    return lax.rem(value, size)


def kernel(
    feat_n, samp_n, lam_total,
    feats, labels, alphas, orders,
    alpha_out, score_out,
    own, shared, lab_all, alp_all, ord_all, part, inbox, full, ghl,
    load_sem, xs_sem, xr_sem, ms_sem, mr_sem, rs_send, rs_recv, ag_send, ag_recv, fw_send, fw_recv,
):
    rows, depth = feats.shape
    width = depth // samp_n
    piece = width // PIECES
    slab_a = part[0].shape[1]
    slab_b = part[1].shape[1] if len(part) > 1 else 0
    slabs = (slab_a, slab_b)
    starts = (0, slab_a)
    me_f, me_s = lax.axis_index("feat"), lax.axis_index("samp")

    barrier = pltpu.get_barrier_semaphore()
    for k in range(1, samp_n):
        pl.semaphore_signal(barrier, inc=1, device_id={"samp": wrap(me_s + k, samp_n)})
    for k in range(1, feat_n):
        pl.semaphore_signal(barrier, inc=1, device_id={"feat": wrap(me_f + k, feat_n)})

    def columns(owner, index):
        return pl.ds(pl.multiple_of(owner * width + index * piece, 128), piece)

    loads = []
    for k in range(samp_n):
        owner = wrap(me_s + k, samp_n)
        for i in range(PIECES):
            target = shared.at[me_s, i] if k == 0 else own.at[k - 1, i]
            loads.append(
                pltpu.make_async_copy(feats.at[:, columns(owner, i)], target, load_sem.at[k * PIECES + i])
            )
    for copy in loads:
        copy.start()
    smalls = ((labels, lab_all), (alphas, alp_all), (orders, ord_all))
    small_loads = [
        pltpu.make_async_copy(source, target.at[me_s], load_sem.at[samp_n * PIECES + n])
        for n, (source, target) in enumerate(smalls)
    ]
    for copy in small_loads:
        copy.start()

    pl.semaphore_wait(barrier, samp_n - 1 + feat_n - 1)

    exchange = []
    for k in range(1, samp_n):
        owner = wrap(me_s + k, samp_n)
        for i in range(PIECES):
            exchange.append(
                pltpu.make_async_remote_copy(
                    feats.at[:, columns(owner, i)], shared.at[me_s, i],
                    xs_sem.at[k - 1, i], xr_sem.at[me_s, i], device_id={"samp": owner},
                )
            )
    for k in range(1, samp_n):
        owner = wrap(me_s + k, samp_n)
        for n, (source, target) in enumerate(smalls):
            exchange.append(
                pltpu.make_async_remote_copy(
                    source, target.at[me_s], ms_sem.at[k - 1, n], mr_sem.at[me_s, n],
                    device_id={"samp": owner},
                )
            )
    for copy in exchange:
        copy.start()

    total = None
    for k in range(samp_n):
        for i in range(PIECES):
            loads[k * PIECES + i].wait()
            block = shared[me_s, i] if k == 0 else own[k - 1, i]
            term = gram_of(block, block)
            total = term if total is None else total + term

    scatter = []

    def scatter_out(group):
        size, start = slabs[group], starts[group]
        for k in range(1, feat_n):
            target = wrap(me_f + k, feat_n)
            copy = pltpu.make_async_remote_copy(
                part[group].at[target], inbox.at[me_f, pl.ds(start, size)],
                rs_send.at[group, k - 1], rs_recv.at[group, me_f], device_id={"feat": target},
            )
            copy.start()
            scatter.append(copy)

    def fill(group, value):
        size = slabs[group]
        count = feat_n * size
        if value.shape[0] < count:
            value = jnp.concatenate(
                [value, jnp.zeros((count - value.shape[0], rows), jnp.float32)], axis=0
            )
        part[group][...] = value.reshape(feat_n, size, rows)

    fill(0, total)
    scatter_out(0)

    pairs = [(p, q) for p in range(samp_n) for q in range(p + 1, samp_n)]
    if pairs:
        cross = [None] * len(pairs)
        for i in range(PIECES):
            for k in range(1, samp_n):
                source = wrap(me_s + k, samp_n)
                pltpu.make_async_copy(
                    shared.at[source, i], shared.at[source, i], xr_sem.at[source, i]
                ).wait()
            for n, (p, q) in enumerate(pairs):
                term = gram_of(shared[p, i], shared[q, i])
                cross[n] = term if cross[n] is None else cross[n] + term
        fill(1, jnp.concatenate(cross, axis=0) if len(cross) > 1 else cross[0])
        scatter_out(1)

    for copy in small_loads:
        copy.wait()
    for k in range(1, samp_n):
        source = wrap(me_s + k, samp_n)
        for n, (_, target) in enumerate(smalls):
            pltpu.make_async_copy(target.at[source], target.at[source], mr_sem.at[source, n]).wait()
    every = range(samp_n)
    signs = [lab_all[p].astype(jnp.float32) for p in every]
    alpha = [alp_all[p] for p in every]
    row_id = lax.broadcasted_iota(jnp.int32, (rows, rows), 0)
    col_id = lax.broadcasted_iota(jnp.int32, (rows, rows), 1)
    place = [
        [
            jnp.sum(
                jnp.where(ord_all[p, r : r + 1, :] == row_id, col_id, 0).astype(jnp.float32),
                axis=1, keepdims=True,
            )
            for p in every
        ]
        for r in range(ROUNDS)
    ]

    for group in range(len(part)):
        inbox[me_f, pl.ds(starts[group], slabs[group])] = part[group][me_f]
        for k in range(1, feat_n):
            source = wrap(me_f + k, feat_n)
            landed = inbox.at[source, pl.ds(starts[group], slabs[group])]
            pltpu.make_async_copy(landed, landed, rs_recv.at[group, source]).wait()
    summed = inbox[0]
    for n in range(1, feat_n):
        summed = summed + inbox[n]
    full[me_s, me_f] = summed
    gather = []
    for k in range(1, feat_n):
        target = wrap(me_f + k, feat_n)
        copy = pltpu.make_async_remote_copy(
            full.at[me_s, me_f], full.at[me_s, me_f],
            ag_send.at[k - 1], ag_recv.at[me_f], device_id={"feat": target},
        )
        copy.start()
        gather.append(copy)
    for k in range(1, feat_n):
        source = wrap(me_f + k, feat_n)
        landed = full.at[me_s, source]
        pltpu.make_async_copy(landed, landed, ag_recv.at[source]).wait()
    forward = []
    for k in range(1, samp_n):
        copy = pltpu.make_async_remote_copy(
            full.at[me_s], full.at[me_s], fw_send.at[k - 1], fw_recv.at[me_s],
            device_id={"samp": wrap(me_s + k, samp_n)},
        )
        copy.start()
        forward.append(copy)
    for k in range(1, samp_n):
        source = wrap(me_s + k, samp_n)
        pltpu.make_async_copy(full.at[source], full.at[source], fw_recv.at[source]).wait()

    def put(p, q, value):
        high = value.astype(jnp.bfloat16)
        low = (value - high.astype(jnp.float32)).astype(jnp.bfloat16)
        ghl[q, pl.ds(p * rows, rows), pl.ds(0, rows)] = high
        ghl[q, pl.ds(p * rows, rows), pl.ds(rows, rows)] = low

    gain = []
    for p in every:
        block = full[p, :, :slab_a, :].reshape(feat_n * slab_a, rows)[:rows]
        put(p, p, block)
        norm = jnp.sum(jnp.where(row_id == col_id, block, 0.0), axis=1, keepdims=True) + 1.0
        gain.append(lam_total / norm)
    if pairs:
        cross_sum = full[0, :, slab_a:, :]
        for s in range(1, samp_n):
            cross_sum = cross_sum + full[s, :, slab_a:, :]
        cross_sum = cross_sum.reshape(feat_n * slab_b, rows)
        for n, (p, q) in enumerate(pairs):
            block = cross_sum[n * rows : (n + 1) * rows]
            put(p, q, block)
            put(q, p, block.T)

    def apply(p, change):
        return jnp.dot(
            ghl[p], jnp.concatenate([change, change], axis=0), preferred_element_type=jnp.float32
        ) * (1.0 / lam_total)

    base = None
    for p in every:
        term = apply(p, (alpha[p] * signs[p]).astype(jnp.bfloat16))
        base = term if base is None else base + term
    for r in range(ROUNDS):
        local = list(alpha)
        coupled = [None] * samp_n
        moved = None
        for b in range(rows // BLOCK):
            for p in every:
                margins = base[p * rows : (p + 1) * rows]
                if coupled[p] is not None:
                    margins = margins + coupled[p]
                updated = jnp.clip(local[p] + gain[p] * (1.0 - signs[p] * margins), 0.0, 1.0)
                inside = (place[r][p] >= b * BLOCK) & (place[r][p] < (b + 1) * BLOCK)
                updated = jnp.where(inside, updated, local[p])
                change = ((updated - local[p]) * signs[p]).astype(jnp.bfloat16)
                local[p] = updated
                term = apply(p, change)
                mine = term[p * rows : (p + 1) * rows]
                coupled[p] = mine if coupled[p] is None else coupled[p] + mine
                moved = term if moved is None else moved + term
        base = base + moved * (1.0 / samp_n)
        alpha = [alpha[p] + (local[p] - alpha[p]) * (1.0 / samp_n) for p in every]

    alpha_mine, score_mine = alpha[0], base[:rows]
    for p in range(1, samp_n):
        alpha_mine = jnp.where(me_s == p, alpha[p], alpha_mine)
        score_mine = jnp.where(me_s == p, base[p * rows : (p + 1) * rows], score_mine)
    alpha_out[...] = alpha_mine
    score_out[...] = score_mine

    for copy in exchange + scatter + gather + forward:
        copy.wait_send()


def per_device(features, labels, alpha_start, order):
    rows, depth = features.shape
    label_n = labels.shape[1]
    feat_n, samp_n = lax.axis_size("feat"), lax.axis_size("samp")
    width = depth // samp_n
    piece = width // PIECES
    pair_n = samp_n * (samp_n - 1) // 2
    sizes = [round_up(-(-rows // feat_n), 8)]
    if pair_n:
        sizes.append(round_up(-(-pair_n * rows // feat_n), 8))
    lam_total = REG_SCALE * depth * feat_n
    dma = pltpu.SemaphoreType.DMA
    others, peers = max(samp_n - 1, 1), max(feat_n - 1, 1)
    return pl.pallas_call(
        functools.partial(kernel, feat_n, samp_n, lam_total),
        out_shape=[jax.ShapeDtypeStruct((rows, label_n), jnp.float32)] * 2,
        in_specs=[pl.BlockSpec(memory_space=pl.ANY)] * 4,
        out_specs=[pl.BlockSpec(memory_space=pltpu.VMEM)] * 2,
        scratch_shapes=[
            pltpu.VMEM((others, PIECES, rows, piece), features.dtype),
            pltpu.VMEM((samp_n, PIECES, rows, piece), features.dtype),
            pltpu.VMEM((samp_n,) + labels.shape, labels.dtype),
            pltpu.VMEM((samp_n,) + alpha_start.shape, jnp.float32),
            pltpu.VMEM((samp_n,) + order.shape, order.dtype),
            [pltpu.VMEM((feat_n, size, rows), jnp.float32) for size in sizes],
            pltpu.VMEM((feat_n, sum(sizes), rows), jnp.float32),
            pltpu.VMEM((samp_n, feat_n, sum(sizes), rows), jnp.float32),
            pltpu.VMEM((samp_n, samp_n * rows, 2 * rows), jnp.bfloat16),
            dma((samp_n * PIECES + 3,)),
            dma((others, PIECES)),
            dma((samp_n, PIECES)),
            dma((others, 3)),
            dma((samp_n, 3)),
            dma((2, peers)),
            dma((2, feat_n)),
            dma((peers,)),
            dma((feat_n,)),
            dma((others,)),
            dma((samp_n,)),
        ],
        compiler_params=pltpu.CompilerParams(
            collective_id=0, has_side_effects=True, vmem_limit_bytes=48 * 1024 * 1024
        ),
    )(features, labels, alpha_start, order)


def solution(mesh):
    return jax.shard_map(
        per_device,
        mesh=mesh,
        in_specs=(P("samp", "feat"), P("samp", None), P("samp", None), P(None, "samp")),
        out_specs=(P("samp", None), P("samp", None)),
        check_vma=False,
    )
```

```python
import functools

import jax
import jax.numpy as jnp
from jax import lax
from jax.experimental import pallas as pl
from jax.experimental.pallas import tpu as pltpu
from jax.sharding import PartitionSpec as P

BLOCK = 64
ROUNDS = 2
REG_SCALE = 0.9
PIECES = 2


def round_up(value, unit):
    return (value + unit - 1) // unit * unit


def gram_of(left, right):
    return lax.dot_general(
        left, right, (((1,), (1,)), ((), ())), preferred_element_type=jnp.float32
    )


def wrap(value, size):
    return lax.rem(value, size)


def kernel(
    feat_n, samp_n, lam_total,
    feats, labels, alphas, orders,
    alpha_out, score_out,
    own, shared, lab_all, alp_all, ord_all, part, inbox, full, ghl,
    load_sem, xs_sem, xr_sem, ms_sem, mr_sem, rs_send, rs_recv, ag_send, ag_recv, fw_send, fw_recv,
):
    rows, depth = feats.shape
    width = depth // samp_n
    piece = width // PIECES
    slab_a = part[0].shape[1]
    slab_b = part[1].shape[1] if len(part) > 1 else 0
    slabs = (slab_a, slab_b)
    starts = (0, slab_a)
    me_f, me_s = lax.axis_index("feat"), lax.axis_index("samp")

    barrier = pltpu.get_barrier_semaphore()
    for k in range(1, samp_n):
        pl.semaphore_signal(barrier, inc=1, device_id={"samp": wrap(me_s + k, samp_n)})
    for k in range(1, feat_n):
        pl.semaphore_signal(barrier, inc=1, device_id={"feat": wrap(me_f + k, feat_n)})

    def columns(owner, index):
        return pl.ds(pl.multiple_of(owner * width + index * piece, 128), piece)

    loads = []
    for k in range(samp_n):
        owner = wrap(me_s + k, samp_n)
        for i in range(PIECES):
            target = shared.at[me_s, i] if k == 0 else own.at[k - 1, i]
            loads.append(
                pltpu.make_async_copy(feats.at[:, columns(owner, i)], target, load_sem.at[k * PIECES + i])
            )
    for copy in loads:
        copy.start()
    smalls = ((labels, lab_all), (alphas, alp_all), (orders, ord_all))
    small_loads = [
        pltpu.make_async_copy(source, target.at[me_s], load_sem.at[samp_n * PIECES + n])
        for n, (source, target) in enumerate(smalls)
    ]
    for copy in small_loads:
        copy.start()

    pl.semaphore_wait(barrier, samp_n - 1 + feat_n - 1)

    exchange = []
    for k in range(1, samp_n):
        owner = wrap(me_s + k, samp_n)
        for i in range(PIECES):
            exchange.append(
                pltpu.make_async_remote_copy(
                    feats.at[:, columns(owner, i)], shared.at[me_s, i],
                    xs_sem.at[k - 1, i], xr_sem.at[me_s, i], device_id={"samp": owner},
                )
            )
    for k in range(1, samp_n):
        owner = wrap(me_s + k, samp_n)
        for n, (source, target) in enumerate(smalls):
            exchange.append(
                pltpu.make_async_remote_copy(
                    source, target.at[me_s], ms_sem.at[k - 1, n], mr_sem.at[me_s, n],
                    device_id={"samp": owner},
                )
            )
    for copy in exchange:
        copy.start()

    total = None
    for k in range(samp_n):
        for i in range(PIECES):
            loads[k * PIECES + i].wait()
            block = shared[me_s, i] if k == 0 else own[k - 1, i]
            term = gram_of(block, block)
            total = term if total is None else total + term

    scatter = []

    def scatter_out(group):
        size, start = slabs[group], starts[group]
        for k in range(1, feat_n):
            target = wrap(me_f + k, feat_n)
            copy = pltpu.make_async_remote_copy(
                part[group].at[target], inbox.at[me_f, pl.ds(start, size)],
                rs_send.at[group, k - 1], rs_recv.at[group, me_f], device_id={"feat": target},
            )
            copy.start()
            scatter.append(copy)

    def fill(group, value):
        size = slabs[group]
        count = feat_n * size
        if value.shape[0] < count:
            value = jnp.concatenate(
                [value, jnp.zeros((count - value.shape[0], rows), jnp.float32)], axis=0
            )
        part[group][...] = value.reshape(feat_n, size, rows)

    fill(0, total)
    scatter_out(0)

    pairs = [(p, q) for p in range(samp_n) for q in range(p + 1, samp_n)]
    if pairs:
        cross = [None] * len(pairs)
        for i in range(PIECES):
            for k in range(1, samp_n):
                source = wrap(me_s + k, samp_n)
                pltpu.make_async_copy(
                    shared.at[source, i], shared.at[source, i], xr_sem.at[source, i]
                ).wait()
            for n, (p, q) in enumerate(pairs):
                term = gram_of(shared[p, i], shared[q, i])
                cross[n] = term if cross[n] is None else cross[n] + term
        fill(1, jnp.concatenate(cross, axis=0) if len(cross) > 1 else cross[0])
        scatter_out(1)

    for copy in small_loads:
        copy.wait()
    for k in range(1, samp_n):
        source = wrap(me_s + k, samp_n)
        for n, (_, target) in enumerate(smalls):
            pltpu.make_async_copy(target.at[source], target.at[source], mr_sem.at[source, n]).wait()
    every = range(samp_n)
    signs = [lab_all[p].astype(jnp.float32) for p in every]
    alpha = [alp_all[p] for p in every]
    row_id = lax.broadcasted_iota(jnp.int32, (rows, rows), 0)
    col_id = lax.broadcasted_iota(jnp.int32, (rows, rows), 1)
    block_id = (lax.broadcasted_iota(jnp.int32, (8, rows), 1) // BLOCK).astype(jnp.bfloat16)
    place = [
        [
            gram_of(
                block_id, jnp.where(ord_all[p, r : r + 1, :] == row_id, 1.0, 0.0).astype(jnp.bfloat16)
            )[:1]
            for p in every
        ]
        for r in range(ROUNDS)
    ]

    for group in range(len(part)):
        inbox[me_f, pl.ds(starts[group], slabs[group])] = part[group][me_f]
        for k in range(1, feat_n):
            source = wrap(me_f + k, feat_n)
            landed = inbox.at[source, pl.ds(starts[group], slabs[group])]
            pltpu.make_async_copy(landed, landed, rs_recv.at[group, source]).wait()
    summed = inbox[0]
    for n in range(1, feat_n):
        summed = summed + inbox[n]
    full[me_s, me_f] = summed
    gather = []
    for k in range(1, feat_n):
        target = wrap(me_f + k, feat_n)
        copy = pltpu.make_async_remote_copy(
            full.at[me_s, me_f], full.at[me_s, me_f],
            ag_send.at[k - 1], ag_recv.at[me_f], device_id={"feat": target},
        )
        copy.start()
        gather.append(copy)
    for k in range(1, feat_n):
        source = wrap(me_f + k, feat_n)
        landed = full.at[me_s, source]
        pltpu.make_async_copy(landed, landed, ag_recv.at[source]).wait()
    forward = []
    for k in range(1, samp_n):
        copy = pltpu.make_async_remote_copy(
            full.at[me_s], full.at[me_s], fw_send.at[k - 1], fw_recv.at[me_s],
            device_id={"samp": wrap(me_s + k, samp_n)},
        )
        copy.start()
        forward.append(copy)
    for k in range(1, samp_n):
        source = wrap(me_s + k, samp_n)
        pltpu.make_async_copy(full.at[source], full.at[source], fw_recv.at[source]).wait()

    def put(p, q, value):
        high = value.astype(jnp.bfloat16)
        low = (value - high.astype(jnp.float32)).astype(jnp.bfloat16)
        ghl[p, pl.ds(0, rows), pl.ds(q * rows, rows)] = high
        ghl[p, pl.ds(rows, rows), pl.ds(q * rows, rows)] = low

    gain = []
    for p in every:
        block = full[p, :, :slab_a, :].reshape(feat_n * slab_a, rows)[:rows]
        put(p, p, block)
        norm = jnp.sum(jnp.where(row_id == col_id, block, 0.0), axis=0, keepdims=True) + 1.0
        gain.append(lam_total / norm)
    if pairs:
        cross_sum = full[0, :, slab_a:, :]
        for s in range(1, samp_n):
            cross_sum = cross_sum + full[s, :, slab_a:, :]
        cross_sum = cross_sum.reshape(feat_n * slab_b, rows)
        for n, (p, q) in enumerate(pairs):
            block = cross_sum[n * rows : (n + 1) * rows]
            put(p, q, block)
            put(q, p, block.T)

    def apply(p, change):
        return jnp.dot(
            jnp.concatenate([change, change], axis=1), ghl[p], preferred_element_type=jnp.float32
        ) * (1.0 / lam_total)

    base = None
    for p in every:
        term = apply(p, (alpha[p] * signs[p]).astype(jnp.bfloat16))
        base = term if base is None else base + term
    for r in range(ROUNDS):
        local = list(alpha)
        coupled = [None] * samp_n
        moved = None
        for b in range(rows // BLOCK):
            for p in every:
                margins = base[:, p * rows : (p + 1) * rows]
                if coupled[p] is not None:
                    margins = margins + coupled[p]
                updated = jnp.clip(local[p] + gain[p] * (1.0 - signs[p] * margins), 0.0, 1.0)
                updated = jnp.where(place[r][p] == float(b), updated, local[p])
                change = ((updated - local[p]) * signs[p]).astype(jnp.bfloat16)
                local[p] = updated
                term = apply(p, change)
                mine = term[:, p * rows : (p + 1) * rows]
                coupled[p] = mine if coupled[p] is None else coupled[p] + mine
                moved = term if moved is None else moved + term
        base = base + moved * (1.0 / samp_n)
        alpha = [alpha[p] + (local[p] - alpha[p]) * (1.0 / samp_n) for p in every]

    alpha_mine, score_mine = alpha[0], base[:, :rows]
    for p in range(1, samp_n):
        alpha_mine = jnp.where(me_s == p, alpha[p], alpha_mine)
        score_mine = jnp.where(me_s == p, base[:, p * rows : (p + 1) * rows], score_mine)
    alpha_out[...] = alpha_mine
    score_out[...] = score_mine

    for copy in exchange + scatter + gather + forward:
        copy.wait_send()


def per_device(features, labels, alpha_start, order):
    rows, depth = features.shape
    label_n = labels.shape[1]
    labels, alpha_start = labels.T, alpha_start.T
    feat_n, samp_n = lax.axis_size("feat"), lax.axis_size("samp")
    width = depth // samp_n
    piece = width // PIECES
    pair_n = samp_n * (samp_n - 1) // 2
    sizes = [round_up(-(-rows // feat_n), 8)]
    if pair_n:
        sizes.append(round_up(-(-pair_n * rows // feat_n), 8))
    lam_total = REG_SCALE * depth * feat_n
    dma = pltpu.SemaphoreType.DMA
    others, peers = max(samp_n - 1, 1), max(feat_n - 1, 1)
    alpha, scores = pl.pallas_call(
        functools.partial(kernel, feat_n, samp_n, lam_total),
        out_shape=[jax.ShapeDtypeStruct((label_n, rows), jnp.float32)] * 2,
        in_specs=[pl.BlockSpec(memory_space=pltpu.HBM)] * 4,
        out_specs=[pl.BlockSpec(memory_space=pltpu.VMEM)] * 2,
        scratch_shapes=[
            pltpu.VMEM((others, PIECES, rows, piece), features.dtype),
            pltpu.VMEM((samp_n, PIECES, rows, piece), features.dtype),
            pltpu.VMEM((samp_n,) + labels.shape, labels.dtype),
            pltpu.VMEM((samp_n,) + alpha_start.shape, jnp.float32),
            pltpu.VMEM((samp_n,) + order.shape, order.dtype),
            [pltpu.VMEM((feat_n, size, rows), jnp.float32) for size in sizes],
            pltpu.VMEM((feat_n, sum(sizes), rows), jnp.float32),
            pltpu.VMEM((samp_n, feat_n, sum(sizes), rows), jnp.float32),
            pltpu.VMEM((samp_n, 2 * rows, samp_n * rows), jnp.bfloat16),
            dma((samp_n * PIECES + 3,)),
            dma((others, PIECES)),
            dma((samp_n, PIECES)),
            dma((others, 3)),
            dma((samp_n, 3)),
            dma((2, peers)),
            dma((2, feat_n)),
            dma((peers,)),
            dma((feat_n,)),
            dma((others,)),
            dma((samp_n,)),
        ],
        compiler_params=pltpu.CompilerParams(
            collective_id=0, has_side_effects=True, vmem_limit_bytes=65000000
        ),
    )(features, labels, alpha_start, order)
    return alpha.T, scores.T


def solution(mesh):
    return jax.shard_map(
        per_device,
        mesh=mesh,
        in_specs=(P("samp", "feat"), P("samp", None), P("samp", None), P(None, "samp")),
        out_specs=(P("samp", None), P("samp", None)),
        check_vma=False,
    )
```

```python
import functools

import jax
import jax.numpy as jnp
from jax import lax
from jax.experimental import pallas as pl
from jax.experimental.pallas import tpu as pltpu
from jax.sharding import PartitionSpec as P

BLOCK = 64
ROUNDS = 2
REG_SCALE = 0.9
PIECES = 2
KINDS = (jnp.float32, jnp.bfloat16)


def round_up(value, unit):
    return (value + unit - 1) // unit * unit


def gram_of(left, right):
    return lax.dot_general(
        left, right, (((1,), (1,)), ((), ())), preferred_element_type=jnp.float32
    )


def wrap(value, size):
    return lax.rem(value, size)


def kernel(
    feat_n, samp_n, lam_total,
    feats, labels, alphas, orders,
    alpha_out, score_out,
    own, shared, lab_all, alp_all, ord_all, part, inbox, full, ghl,
    here_sem, group_sem, go_sem, load_sem, xs_sem, xr_sem, ms_sem, mr_sem, rs_send, rs_recv, ag_send, ag_recv, fw_send, fw_recv,
):
    rows, depth = feats.shape
    width = depth // samp_n
    piece = width // PIECES
    slab_a = part[0].shape[1]
    slab_b = part[1].shape[1] if len(part) > 1 else 0
    slabs = (slab_a, slab_b)
    lead = samp_n - 1
    me_f, me_s = lax.axis_index("feat"), lax.axis_index("samp")

    barrier = pltpu.get_barrier_semaphore()
    def columns(owner, index):
        return pl.ds(pl.multiple_of(owner * width + index * piece, 128), piece)

    loads = []
    for k in range(samp_n):
        owner = wrap(me_s + k, samp_n)
        for i in range(PIECES):
            target = shared.at[me_s, i] if k == 0 else own.at[k - 1, i]
            loads.append(
                pltpu.make_async_copy(feats.at[:, columns(owner, i)], target, load_sem.at[k * PIECES + i])
            )
    for copy in loads:
        copy.start()
    smalls = ((labels, lab_all), (alphas, alp_all), (orders, ord_all))
    small_loads = [
        pltpu.make_async_copy(source, target.at[me_s], load_sem.at[samp_n * PIECES + n])
        for n, (source, target) in enumerate(smalls)
    ]
    for copy in small_loads:
        copy.start()

    if samp_n > 1:
        @pl.when(me_s == lead)
        def _():
            for q in range(samp_n - 1):
                pl.semaphore_signal(barrier, inc=1, device_id={"samp": q})

        @pl.when(me_s != lead)
        def _():
            pl.semaphore_wait(barrier, 1)
            pl.semaphore_signal(here_sem, inc=1, device_id={"samp": lead})

    @pl.when(me_s == lead)
    def _():
        if samp_n > 1:
            pl.semaphore_wait(here_sem, samp_n - 1)
        for k in range(1, feat_n):
            pl.semaphore_signal(barrier, inc=1, device_id={"feat": wrap(me_f + k, feat_n)})
        if samp_n > 2:
            for q in range(samp_n - 1):
                pl.semaphore_signal(group_sem, inc=1, device_id={"samp": q})

    if samp_n > 2:
        @pl.when(me_s != lead)
        def _():
            pl.semaphore_wait(group_sem, 1)

    exchange = []
    for k in range(1, samp_n):
        owner = wrap(me_s + k, samp_n)
        for i in range(PIECES):
            exchange.append(
                pltpu.make_async_remote_copy(
                    feats.at[:, columns(owner, i)], shared.at[me_s, i],
                    xs_sem.at[k - 1, i], xr_sem.at[me_s, i], device_id={"samp": owner},
                )
            )
    for k in range(1, samp_n):
        owner = wrap(me_s + k, samp_n)
        for n, (source, target) in enumerate(smalls):
            exchange.append(
                pltpu.make_async_remote_copy(
                    source, target.at[me_s], ms_sem.at[k - 1, n], mr_sem.at[me_s, n],
                    device_id={"samp": owner},
                )
            )
    for copy in exchange:
        copy.start()

    total = None
    for k in range(samp_n):
        for i in range(PIECES):
            loads[k * PIECES + i].wait()
            block = shared[me_s, i] if k == 0 else own[k - 1, i]
            term = gram_of(block, block)
            total = term if total is None else total + term

    @pl.when(me_s == lead)
    def _():
        if feat_n > 1:
            pl.semaphore_wait(barrier, feat_n - 1)
        for q in range(samp_n - 1):
            pl.semaphore_signal(go_sem, inc=1, device_id={"samp": q})

    if samp_n > 1:
        @pl.when(me_s != lead)
        def _():
            pl.semaphore_wait(go_sem, 1)

    scatter = []

    def scatter_out(group):
        for k in range(1, feat_n):
            target = wrap(me_f + k, feat_n)
            copy = pltpu.make_async_remote_copy(
                part[group].at[target], inbox[group].at[me_f],
                rs_send.at[group, k - 1], rs_recv.at[group, me_f], device_id={"feat": target},
            )
            copy.start()
            scatter.append(copy)

    def fill(group, value):
        size = slabs[group]
        count = feat_n * size
        if value.shape[0] < count:
            value = jnp.concatenate(
                [value, jnp.zeros((count - value.shape[0], rows), jnp.float32)], axis=0
            )
        part[group][...] = value.reshape(feat_n, size, rows).astype(part[group].dtype)

    fill(0, total)
    scatter_out(0)

    pairs = [(p, q) for p in range(samp_n) for q in range(p + 1, samp_n)]
    if pairs:
        cross = [None] * len(pairs)
        for i in range(PIECES):
            for k in range(1, samp_n):
                source = wrap(me_s + k, samp_n)
                pltpu.make_async_copy(
                    shared.at[source, i], shared.at[source, i], xr_sem.at[source, i]
                ).wait()
            for n, (p, q) in enumerate(pairs):
                term = gram_of(shared[p, i], shared[q, i])
                cross[n] = term if cross[n] is None else cross[n] + term
        fill(1, jnp.concatenate(cross, axis=0) if len(cross) > 1 else cross[0])
        scatter_out(1)

    for copy in small_loads:
        copy.wait()
    for k in range(1, samp_n):
        source = wrap(me_s + k, samp_n)
        for n, (_, target) in enumerate(smalls):
            pltpu.make_async_copy(target.at[source], target.at[source], mr_sem.at[source, n]).wait()
    every = range(samp_n)
    signs = [lab_all[p].astype(jnp.float32) for p in every]
    alpha = [alp_all[p] for p in every]
    row_id = lax.broadcasted_iota(jnp.int32, (rows, rows), 0)
    col_id = lax.broadcasted_iota(jnp.int32, (rows, rows), 1)
    block_id = (lax.broadcasted_iota(jnp.int32, (8, rows), 1) // BLOCK).astype(jnp.bfloat16)
    place = [
        [
            gram_of(
                block_id, jnp.where(ord_all[p, r : r + 1, :] == row_id, 1.0, 0.0).astype(jnp.bfloat16)
            )[:1]
            for p in every
        ]
        for r in range(ROUNDS)
    ]

    gather, forward = [], []

    def sum_and_gather(group):
        inbox[group][me_f] = part[group][me_f]
        for k in range(1, feat_n):
            landed = inbox[group].at[wrap(me_f + k, feat_n)]
            pltpu.make_async_copy(landed, landed, rs_recv.at[group, wrap(me_f + k, feat_n)]).wait()
        summed = inbox[group][0].astype(jnp.float32)
        for n in range(1, feat_n):
            summed = summed + inbox[group][n].astype(jnp.float32)
        full[group][me_s, me_f] = summed.astype(full[group].dtype)
        for k in range(1, feat_n):
            copy = pltpu.make_async_remote_copy(
                full[group].at[me_s, me_f], full[group].at[me_s, me_f],
                ag_send.at[group, k - 1], ag_recv.at[group, me_f],
                device_id={"feat": wrap(me_f + k, feat_n)},
            )
            copy.start()
            gather.append(copy)

    def pass_on(group):
        for k in range(1, feat_n):
            source = wrap(me_f + k, feat_n)
            landed = full[group].at[me_s, source]
            pltpu.make_async_copy(landed, landed, ag_recv.at[group, source]).wait()
        for k in range(1, samp_n):
            copy = pltpu.make_async_remote_copy(
                full[group].at[me_s], full[group].at[me_s],
                fw_send.at[group, k - 1], fw_recv.at[group, me_s],
                device_id={"samp": wrap(me_s + k, samp_n)},
            )
            copy.start()
            forward.append(copy)

    def arrived(group):
        for k in range(1, samp_n):
            source = wrap(me_s + k, samp_n)
            landed = full[group].at[source]
            pltpu.make_async_copy(landed, landed, fw_recv.at[group, source]).wait()

    groups = range(len(part))
    for group in groups:
        sum_and_gather(group)
    for group in groups:
        pass_on(group)
    arrived(0)

    def put(p, q, value):
        high = value.astype(jnp.bfloat16)
        low = (value - high.astype(jnp.float32)).astype(jnp.bfloat16)
        ghl[p, pl.ds(0, rows), pl.ds(q * rows, rows)] = high
        ghl[p, pl.ds(rows, rows), pl.ds(q * rows, rows)] = low

    gain = []
    for p in every:
        block = full[0][p].reshape(feat_n * slab_a, rows)[:rows]
        put(p, p, block)
        norm = jnp.sum(jnp.where(row_id == col_id, block, 0.0), axis=0, keepdims=True) + 1.0
        gain.append(lam_total / norm)
    if pairs:
        arrived(1)
        cross_sum = full[1][0].astype(jnp.float32)
        for s in range(1, samp_n):
            cross_sum = cross_sum + full[1][s].astype(jnp.float32)
        cross_sum = cross_sum.reshape(feat_n * slab_b, rows)
        for n, (p, q) in enumerate(pairs):
            block = cross_sum[n * rows : (n + 1) * rows]
            put(p, q, block)
            put(q, p, block.T)

    def apply(p, change):
        return jnp.dot(
            jnp.concatenate([change, change], axis=1), ghl[p], preferred_element_type=jnp.float32
        ) * (1.0 / lam_total)

    base = None
    for p in every:
        term = apply(p, (alpha[p] * signs[p]).astype(jnp.bfloat16))
        base = term if base is None else base + term
    for r in range(ROUNDS):
        local = list(alpha)
        coupled = [None] * samp_n
        moved = None
        for b in range(rows // BLOCK):
            for p in every:
                margins = base[:, p * rows : (p + 1) * rows]
                if coupled[p] is not None:
                    margins = margins + coupled[p]
                updated = jnp.clip(local[p] + gain[p] * (1.0 - signs[p] * margins), 0.0, 1.0)
                updated = jnp.where(place[r][p] == float(b), updated, local[p])
                change = ((updated - local[p]) * signs[p]).astype(jnp.bfloat16)
                local[p] = updated
                term = apply(p, change)
                mine = term[:, p * rows : (p + 1) * rows]
                coupled[p] = mine if coupled[p] is None else coupled[p] + mine
                moved = term if moved is None else moved + term
        base = base + moved * (1.0 / samp_n)
        alpha = [alpha[p] + (local[p] - alpha[p]) * (1.0 / samp_n) for p in every]

    alpha_mine, score_mine = alpha[0], base[:, :rows]
    for p in range(1, samp_n):
        alpha_mine = jnp.where(me_s == p, alpha[p], alpha_mine)
        score_mine = jnp.where(me_s == p, base[:, p * rows : (p + 1) * rows], score_mine)
    alpha_out[...] = alpha_mine
    score_out[...] = score_mine

    for copy in exchange + scatter + gather + forward:
        copy.wait_send()


def per_device(features, labels, alpha_start, order):
    rows, depth = features.shape
    label_n = labels.shape[1]
    labels, alpha_start = labels.T, alpha_start.T
    feat_n, samp_n = lax.axis_size("feat"), lax.axis_size("samp")
    width = depth // samp_n
    piece = width // PIECES
    pair_n = samp_n * (samp_n - 1) // 2
    sizes = [round_up(-(-rows // feat_n), 8)]
    if pair_n:
        sizes.append(round_up(-(-pair_n * rows // feat_n), 8))
    lam_total = REG_SCALE * depth * feat_n
    dma = pltpu.SemaphoreType.DMA
    others, peers = max(samp_n - 1, 1), max(feat_n - 1, 1)
    alpha, scores = pl.pallas_call(
        functools.partial(kernel, feat_n, samp_n, lam_total),
        out_shape=[jax.ShapeDtypeStruct((label_n, rows), jnp.float32)] * 2,
        in_specs=[pl.BlockSpec(memory_space=pltpu.HBM)] * 4,
        out_specs=[pl.BlockSpec(memory_space=pltpu.VMEM)] * 2,
        scratch_shapes=[
            pltpu.VMEM((others, PIECES, rows, piece), features.dtype),
            pltpu.VMEM((samp_n, PIECES, rows, piece), features.dtype),
            pltpu.VMEM((samp_n,) + labels.shape, labels.dtype),
            pltpu.VMEM((samp_n,) + alpha_start.shape, jnp.float32),
            pltpu.VMEM((samp_n,) + order.shape, order.dtype),
            [pltpu.VMEM((feat_n, size, rows), kind) for size, kind in zip(sizes, KINDS)],
            [pltpu.VMEM((feat_n, size, rows), kind) for size, kind in zip(sizes, KINDS)],
            [pltpu.VMEM((samp_n, feat_n, size, rows), kind) for size, kind in zip(sizes, KINDS)],
            pltpu.VMEM((samp_n, 2 * rows, samp_n * rows), jnp.bfloat16),
            pltpu.SemaphoreType.REGULAR,
            pltpu.SemaphoreType.REGULAR,
            pltpu.SemaphoreType.REGULAR,
            dma((samp_n * PIECES + 3,)),
            dma((others, PIECES)),
            dma((samp_n, PIECES)),
            dma((others, 3)),
            dma((samp_n, 3)),
            dma((2, peers)),
            dma((2, feat_n)),
            dma((2, peers)),
            dma((2, feat_n)),
            dma((2, others)),
            dma((2, samp_n)),
        ],
        compiler_params=pltpu.CompilerParams(
            collective_id=0, has_side_effects=True, vmem_limit_bytes=56000000
        ),
    )(features, labels, alpha_start, order)
    return alpha.T, scores.T


def solution(mesh):
    return jax.shard_map(
        per_device,
        mesh=mesh,
        in_specs=(P("samp", "feat"), P("samp", None), P("samp", None), P(None, "samp")),
        out_specs=(P("samp", None), P("samp", None)),
        check_vma=False,
    )
```

```python
import functools

import jax
import jax.numpy as jnp
from jax import lax
from jax.experimental import pallas as pl
from jax.experimental.pallas import tpu as pltpu
from jax.sharding import PartitionSpec as P

BLOCK = 64
ROUNDS = 2
REG_SCALE = 0.9
PIECES = 2
KINDS = (jnp.float32, jnp.bfloat16)


def round_up(value, unit):
    return (value + unit - 1) // unit * unit


def gram_of(left, right):
    return lax.dot_general(
        left, right, (((1,), (1,)), ((), ())), preferred_element_type=jnp.float32
    )


def wrap(value, size):
    return lax.rem(value, size)


def kernel(
    feat_n, samp_n, lam_total,
    feats, labels, alphas, orders,
    alpha_out, score_out,
    own, shared, lab_all, alp_all, ord_all, part, inbox, full, ghl,
    here_sem, group_sem, go_sem, load_sem, xs_sem, xr_sem, ms_sem, mr_sem, rs_send, rs_recv, ag_send, ag_recv, fw_send, fw_recv,
):
    rows, depth = feats.shape
    width = depth // samp_n
    piece = width // PIECES
    slab_a = part[0].shape[1]
    slab_b = part[1].shape[1] if len(part) > 1 else 0
    slabs = (slab_a, slab_b)
    lead = samp_n - 1
    me_f, me_s = lax.axis_index("feat"), lax.axis_index("samp")

    barrier = pltpu.get_barrier_semaphore()
    def columns(owner, index):
        return pl.ds(pl.multiple_of(owner * width + index * piece, 128), piece)

    loads = []
    for k in range(samp_n):
        owner = wrap(me_s + k, samp_n)
        for i in range(PIECES):
            target = shared.at[me_s, i] if k == 0 else own.at[k - 1, i]
            loads.append(
                pltpu.make_async_copy(feats.at[:, columns(owner, i)], target, load_sem.at[k * PIECES + i])
            )
    for copy in loads:
        copy.start()
    smalls = ((labels, lab_all), (alphas, alp_all), (orders, ord_all))
    small_loads = [
        pltpu.make_async_copy(source, target.at[me_s], load_sem.at[samp_n * PIECES + n])
        for n, (source, target) in enumerate(smalls)
    ]
    for copy in small_loads:
        copy.start()

    if samp_n > 1:
        @pl.when(me_s == lead)
        def _():
            for q in range(samp_n - 1):
                pl.semaphore_signal(barrier, inc=1, device_id={"samp": q})

        @pl.when(me_s != lead)
        def _():
            pl.semaphore_wait(barrier, 1)
            pl.semaphore_signal(here_sem, inc=1, device_id={"samp": lead})

    @pl.when(me_s == lead)
    def _():
        if samp_n > 1:
            pl.semaphore_wait(here_sem, samp_n - 1)
        for k in range(1, feat_n):
            pl.semaphore_signal(barrier, inc=1, device_id={"feat": wrap(me_f + k, feat_n)})
        if samp_n > 2:
            for q in range(samp_n - 1):
                pl.semaphore_signal(group_sem, inc=1, device_id={"samp": q})

    if samp_n > 2:
        @pl.when(me_s != lead)
        def _():
            pl.semaphore_wait(group_sem, 1)

    exchange = []
    for k in range(1, samp_n):
        owner = wrap(me_s + k, samp_n)
        for i in range(PIECES):
            exchange.append(
                pltpu.make_async_remote_copy(
                    feats.at[:, columns(owner, i)], shared.at[me_s, i],
                    xs_sem.at[k - 1, i], xr_sem.at[me_s, i], device_id={"samp": owner},
                )
            )
    for k in range(1, samp_n):
        owner = wrap(me_s + k, samp_n)
        for n, (source, target) in enumerate(smalls):
            exchange.append(
                pltpu.make_async_remote_copy(
                    source, target.at[me_s], ms_sem.at[k - 1, n], mr_sem.at[me_s, n],
                    device_id={"samp": owner},
                )
            )
    for copy in exchange:
        copy.start()

    total = None
    for k in range(samp_n):
        for i in range(PIECES):
            loads[k * PIECES + i].wait()
            block = shared[me_s, i] if k == 0 else own[k - 1, i]
            term = gram_of(block, block)
            total = term if total is None else total + term

    scatter = []

    def scatter_out(group):
        for k in range(1, feat_n):
            target = wrap(me_f + k, feat_n)
            copy = pltpu.make_async_remote_copy(
                part[group].at[target], inbox[group].at[me_f],
                rs_send.at[group, k - 1], rs_recv.at[group, me_f], device_id={"feat": target},
            )
            copy.start()
            scatter.append(copy)

    def fill(group, value):
        size = slabs[group]
        count = feat_n * size
        if value.shape[0] < count:
            value = jnp.concatenate(
                [value, jnp.zeros((count - value.shape[0], rows), jnp.float32)], axis=0
            )
        part[group][...] = value.reshape(feat_n, size, rows).astype(part[group].dtype)

    fill(0, total)

    pairs = [(p, q) for p in range(samp_n) for q in range(p + 1, samp_n)]
    if pairs:
        cross = [None] * len(pairs)
        for i in range(PIECES):
            for k in range(1, samp_n):
                source = wrap(me_s + k, samp_n)
                pltpu.make_async_copy(
                    shared.at[source, i], shared.at[source, i], xr_sem.at[source, i]
                ).wait()
            for n, (p, q) in enumerate(pairs):
                term = gram_of(shared[p, i], shared[q, i])
                cross[n] = term if cross[n] is None else cross[n] + term
        fill(1, jnp.concatenate(cross, axis=0) if len(cross) > 1 else cross[0])

    @pl.when(me_s == lead)
    def _():
        if feat_n > 1:
            pl.semaphore_wait(barrier, feat_n - 1)
        for q in range(samp_n - 1):
            pl.semaphore_signal(go_sem, inc=1, device_id={"samp": q})

    if samp_n > 1:
        @pl.when(me_s != lead)
        def _():
            pl.semaphore_wait(go_sem, 1)

    for group in reversed(range(len(part))):
        scatter_out(group)

    for copy in small_loads:
        copy.wait()
    for k in range(1, samp_n):
        source = wrap(me_s + k, samp_n)
        for n, (_, target) in enumerate(smalls):
            pltpu.make_async_copy(target.at[source], target.at[source], mr_sem.at[source, n]).wait()
    every = range(samp_n)
    signs = [lab_all[p].astype(jnp.float32) for p in every]
    alpha = [alp_all[p] for p in every]
    row_id = lax.broadcasted_iota(jnp.int32, (rows, rows), 0)
    col_id = lax.broadcasted_iota(jnp.int32, (rows, rows), 1)
    block_id = (lax.broadcasted_iota(jnp.int32, (8, rows), 1) // BLOCK).astype(jnp.bfloat16)
    place = [
        [
            gram_of(
                block_id, jnp.where(ord_all[p, r : r + 1, :] == row_id, 1.0, 0.0).astype(jnp.bfloat16)
            )[:1]
            for p in every
        ]
        for r in range(ROUNDS)
    ]

    gather, forward = [], []

    def sum_and_gather(group):
        inbox[group][me_f] = part[group][me_f]
        for k in range(1, feat_n):
            landed = inbox[group].at[wrap(me_f + k, feat_n)]
            pltpu.make_async_copy(landed, landed, rs_recv.at[group, wrap(me_f + k, feat_n)]).wait()
        summed = inbox[group][0].astype(jnp.float32)
        for n in range(1, feat_n):
            summed = summed + inbox[group][n].astype(jnp.float32)
        full[group][me_s, me_f] = summed.astype(full[group].dtype)
        for k in range(1, feat_n):
            copy = pltpu.make_async_remote_copy(
                full[group].at[me_s, me_f], full[group].at[me_s, me_f],
                ag_send.at[group, k - 1], ag_recv.at[group, me_f],
                device_id={"feat": wrap(me_f + k, feat_n)},
            )
            copy.start()
            gather.append(copy)

    def pass_on(group):
        for k in range(1, feat_n):
            source = wrap(me_f + k, feat_n)
            landed = full[group].at[me_s, source]
            pltpu.make_async_copy(landed, landed, ag_recv.at[group, source]).wait()
        for k in range(1, samp_n):
            copy = pltpu.make_async_remote_copy(
                full[group].at[me_s], full[group].at[me_s],
                fw_send.at[group, k - 1], fw_recv.at[group, me_s],
                device_id={"samp": wrap(me_s + k, samp_n)},
            )
            copy.start()
            forward.append(copy)

    def arrived(group):
        for k in range(1, samp_n):
            source = wrap(me_s + k, samp_n)
            landed = full[group].at[source]
            pltpu.make_async_copy(landed, landed, fw_recv.at[group, source]).wait()

    groups = range(len(part))
    for group in groups:
        sum_and_gather(group)
    for group in groups:
        pass_on(group)
    arrived(0)

    def put(p, q, value):
        high = value.astype(jnp.bfloat16)
        low = (value - high.astype(jnp.float32)).astype(jnp.bfloat16)
        ghl[p, pl.ds(0, rows), pl.ds(q * rows, rows)] = high
        ghl[p, pl.ds(rows, rows), pl.ds(q * rows, rows)] = low

    gain = []
    for p in every:
        block = full[0][p].reshape(feat_n * slab_a, rows)[:rows]
        put(p, p, block)
        norm = jnp.sum(jnp.where(row_id == col_id, block, 0.0), axis=0, keepdims=True) + 1.0
        gain.append(lam_total / norm)
    if pairs:
        arrived(1)
        cross_sum = full[1][0].astype(jnp.float32)
        for s in range(1, samp_n):
            cross_sum = cross_sum + full[1][s].astype(jnp.float32)
        cross_sum = cross_sum.reshape(feat_n * slab_b, rows)
        for n, (p, q) in enumerate(pairs):
            block = cross_sum[n * rows : (n + 1) * rows]
            put(p, q, block)
            put(q, p, block.T)

    def apply(p, change):
        return jnp.dot(
            jnp.concatenate([change, change], axis=1), ghl[p], preferred_element_type=jnp.float32
        ) * (1.0 / lam_total)

    base = None
    for p in every:
        term = apply(p, (alpha[p] * signs[p]).astype(jnp.bfloat16))
        base = term if base is None else base + term
    for r in range(ROUNDS):
        local = list(alpha)
        coupled = [None] * samp_n
        moved = None
        for b in range(rows // BLOCK):
            for p in every:
                margins = base[:, p * rows : (p + 1) * rows]
                if coupled[p] is not None:
                    margins = margins + coupled[p]
                updated = jnp.clip(local[p] + gain[p] * (1.0 - signs[p] * margins), 0.0, 1.0)
                updated = jnp.where(place[r][p] == float(b), updated, local[p])
                change = ((updated - local[p]) * signs[p]).astype(jnp.bfloat16)
                local[p] = updated
                term = apply(p, change)
                mine = term[:, p * rows : (p + 1) * rows]
                coupled[p] = mine if coupled[p] is None else coupled[p] + mine
                moved = term if moved is None else moved + term
        base = base + moved * (1.0 / samp_n)
        alpha = [alpha[p] + (local[p] - alpha[p]) * (1.0 / samp_n) for p in every]

    alpha_mine, score_mine = alpha[0], base[:, :rows]
    for p in range(1, samp_n):
        alpha_mine = jnp.where(me_s == p, alpha[p], alpha_mine)
        score_mine = jnp.where(me_s == p, base[:, p * rows : (p + 1) * rows], score_mine)
    alpha_out[...] = alpha_mine
    score_out[...] = score_mine

    for copy in exchange + scatter + gather + forward:
        copy.wait_send()


def per_device(features, labels, alpha_start, order):
    rows, depth = features.shape
    label_n = labels.shape[1]
    labels, alpha_start = labels.T, alpha_start.T
    feat_n, samp_n = lax.axis_size("feat"), lax.axis_size("samp")
    width = depth // samp_n
    piece = width // PIECES
    pair_n = samp_n * (samp_n - 1) // 2
    sizes = [round_up(-(-rows // feat_n), 8)]
    if pair_n:
        sizes.append(round_up(-(-pair_n * rows // feat_n), 8))
    lam_total = REG_SCALE * depth * feat_n
    dma = pltpu.SemaphoreType.DMA
    others, peers = max(samp_n - 1, 1), max(feat_n - 1, 1)
    alpha, scores = pl.pallas_call(
        functools.partial(kernel, feat_n, samp_n, lam_total),
        out_shape=[jax.ShapeDtypeStruct((label_n, rows), jnp.float32)] * 2,
        in_specs=[pl.BlockSpec(memory_space=pltpu.HBM)] * 4,
        out_specs=[pl.BlockSpec(memory_space=pltpu.VMEM)] * 2,
        scratch_shapes=[
            pltpu.VMEM((others, PIECES, rows, piece), features.dtype),
            pltpu.VMEM((samp_n, PIECES, rows, piece), features.dtype),
            pltpu.VMEM((samp_n,) + labels.shape, labels.dtype),
            pltpu.VMEM((samp_n,) + alpha_start.shape, jnp.float32),
            pltpu.VMEM((samp_n,) + order.shape, order.dtype),
            [pltpu.VMEM((feat_n, size, rows), kind) for size, kind in zip(sizes, KINDS)],
            [pltpu.VMEM((feat_n, size, rows), kind) for size, kind in zip(sizes, KINDS)],
            [pltpu.VMEM((samp_n, feat_n, size, rows), kind) for size, kind in zip(sizes, KINDS)],
            pltpu.VMEM((samp_n, 2 * rows, samp_n * rows), jnp.bfloat16),
            pltpu.SemaphoreType.REGULAR,
            pltpu.SemaphoreType.REGULAR,
            pltpu.SemaphoreType.REGULAR,
            dma((samp_n * PIECES + 3,)),
            dma((others, PIECES)),
            dma((samp_n, PIECES)),
            dma((others, 3)),
            dma((samp_n, 3)),
            dma((2, peers)),
            dma((2, feat_n)),
            dma((2, peers)),
            dma((2, feat_n)),
            dma((2, others)),
            dma((2, samp_n)),
        ],
        compiler_params=pltpu.CompilerParams(
            collective_id=0, has_side_effects=True, vmem_limit_bytes=56000000
        ),
    )(*(pltpu.with_memory_space_constraint(x, pltpu.HBM) for x in (features, labels, alpha_start, order)))
    return alpha.T, scores.T


def solution(mesh):
    return jax.shard_map(
        per_device,
        mesh=mesh,
        in_specs=(P("samp", "feat"), P("samp", None), P("samp", None), P(None, "samp")),
        out_specs=(P("samp", None), P("samp", None)),
        check_vma=False,
    )
```

```python
import functools

import jax
import jax.numpy as jnp
from jax import lax
from jax.experimental import pallas as pl
from jax.experimental.pallas import tpu as pltpu
from jax.sharding import PartitionSpec as P

BLOCK = 64
ROUNDS = 2
REG_SCALE = 0.9
PIECES = 2
KINDS = (jnp.float32, jnp.bfloat16)


def round_up(value, unit):
    return (value + unit - 1) // unit * unit


def gram_of(left, right):
    return lax.dot_general(
        left, right, (((1,), (1,)), ((), ())), preferred_element_type=jnp.float32
    )


def wrap(value, size):
    return lax.rem(value, size)


def kernel(
    feat_n, samp_n, lam_total,
    feats, labels, alphas, orders,
    alpha_out, score_out,
    own, shared, lab_all, alp_all, ord_all, part, inbox, full, ghl,
    here_sem, group_sem, go_sem, load_sem, xs_sem, xr_sem, ms_sem, mr_sem, rs_send, rs_recv, ag_send, ag_recv, fw_send, fw_recv,
):
    rows, depth = feats.shape
    width = depth // samp_n
    piece = width // PIECES
    slab_a = part[0].shape[1]
    slab_b = part[1].shape[1] if len(part) > 1 else 0
    slabs = (slab_a, slab_b)
    lead = samp_n - 1
    me_f, me_s = lax.axis_index("feat"), lax.axis_index("samp")

    barrier = pltpu.get_barrier_semaphore()
    def columns(owner, index):
        return pl.ds(pl.multiple_of(owner * width + index * piece, 128), piece)

    loads = []
    for k in range(samp_n):
        owner = wrap(me_s + k, samp_n)
        for i in range(PIECES):
            target = shared.at[me_s, i] if k == 0 else own.at[k - 1, i]
            loads.append(
                pltpu.make_async_copy(feats.at[:, columns(owner, i)], target, load_sem.at[k * PIECES + i])
            )
    for copy in loads:
        copy.start()
    smalls = ((labels, lab_all), (alphas, alp_all), (orders, ord_all))
    small_loads = [
        pltpu.make_async_copy(source, target.at[me_s], load_sem.at[samp_n * PIECES + n])
        for n, (source, target) in enumerate(smalls)
    ]
    for copy in small_loads:
        copy.start()

    if samp_n > 1:
        @pl.when(me_s == lead)
        def _():
            for q in range(samp_n - 1):
                pl.semaphore_signal(barrier, inc=1, device_id={"samp": q})

        @pl.when(me_s != lead)
        def _():
            pl.semaphore_wait(barrier, 1)
            pl.semaphore_signal(here_sem, inc=1, device_id={"samp": lead})

    @pl.when(me_s == lead)
    def _():
        if samp_n > 1:
            pl.semaphore_wait(here_sem, samp_n - 1)
        for k in range(1, feat_n):
            pl.semaphore_signal(barrier, inc=1, device_id={"feat": wrap(me_f + k, feat_n)})
        if samp_n > 2:
            for q in range(samp_n - 1):
                pl.semaphore_signal(group_sem, inc=1, device_id={"samp": q})

    if samp_n > 2:
        @pl.when(me_s != lead)
        def _():
            pl.semaphore_wait(group_sem, 1)

    exchange = []
    for k in range(1, samp_n):
        owner = wrap(me_s + k, samp_n)
        for i in range(PIECES):
            exchange.append(
                pltpu.make_async_remote_copy(
                    feats.at[:, columns(owner, i)], shared.at[me_s, i],
                    xs_sem.at[k - 1, i], xr_sem.at[me_s, i], device_id={"samp": owner},
                )
            )
    for k in range(1, samp_n):
        owner = wrap(me_s + k, samp_n)
        for n, (source, target) in enumerate(smalls):
            exchange.append(
                pltpu.make_async_remote_copy(
                    source, target.at[me_s], ms_sem.at[k - 1, n], mr_sem.at[me_s, n],
                    device_id={"samp": owner},
                )
            )
    for copy in exchange:
        copy.start()

    total = None
    for k in range(samp_n):
        for i in range(PIECES):
            loads[k * PIECES + i].wait()
            block = shared[me_s, i] if k == 0 else own[k - 1, i]
            term = gram_of(block, block)
            total = term if total is None else total + term

    scatter = []

    def scatter_out(group):
        for k in range(1, feat_n):
            target = wrap(me_f + k, feat_n)
            copy = pltpu.make_async_remote_copy(
                part[group].at[target], inbox[group].at[me_f],
                rs_send.at[group, k - 1], rs_recv.at[group, me_f], device_id={"feat": target},
            )
            copy.start()
            scatter.append(copy)

    def fill(group, value):
        size = slabs[group]
        count = feat_n * size
        if value.shape[0] < count:
            value = jnp.concatenate(
                [value, jnp.zeros((count - value.shape[0], rows), jnp.float32)], axis=0
            )
        part[group][...] = value.reshape(feat_n, size, rows).astype(part[group].dtype)

    fill(0, total)

    pairs = [(p, q) for p in range(samp_n) for q in range(p + 1, samp_n)]
    if pairs:
        cross = [None] * len(pairs)
        for i in range(PIECES):
            for k in range(1, samp_n):
                source = wrap(me_s + k, samp_n)
                pltpu.make_async_copy(
                    shared.at[source, i], shared.at[source, i], xr_sem.at[source, i]
                ).wait()
            for n, (p, q) in enumerate(pairs):
                term = gram_of(shared[p, i], shared[q, i])
                cross[n] = term if cross[n] is None else cross[n] + term
        fill(1, jnp.concatenate(cross, axis=0) if len(cross) > 1 else cross[0])

    @pl.when(me_s == lead)
    def _():
        if feat_n > 1:
            pl.semaphore_wait(barrier, feat_n - 1)
        for q in range(samp_n - 1):
            pl.semaphore_signal(go_sem, inc=1, device_id={"samp": q})

    if samp_n > 1:
        @pl.when(me_s != lead)
        def _():
            pl.semaphore_wait(go_sem, 1)

    for group in range(len(part)):
        scatter_out(group)

    for copy in small_loads:
        copy.wait()
    for k in range(1, samp_n):
        source = wrap(me_s + k, samp_n)
        for n, (_, target) in enumerate(smalls):
            pltpu.make_async_copy(target.at[source], target.at[source], mr_sem.at[source, n]).wait()
    every = range(samp_n)
    signs = [lab_all[p].astype(jnp.float32) for p in every]
    alpha = [alp_all[p] for p in every]
    row_id = lax.broadcasted_iota(jnp.int32, (rows, rows), 0)
    col_id = lax.broadcasted_iota(jnp.int32, (rows, rows), 1)
    block_id = (lax.broadcasted_iota(jnp.int32, (8, rows), 1) // BLOCK).astype(jnp.bfloat16)
    place = [
        [
            gram_of(
                block_id, jnp.where(ord_all[p, r : r + 1, :] == row_id, 1.0, 0.0).astype(jnp.bfloat16)
            )[:1]
            for p in every
        ]
        for r in range(ROUNDS)
    ]

    gather, forward = [], []

    def sum_and_gather(group):
        inbox[group][me_f] = part[group][me_f]
        for k in range(1, feat_n):
            landed = inbox[group].at[wrap(me_f + k, feat_n)]
            pltpu.make_async_copy(landed, landed, rs_recv.at[group, wrap(me_f + k, feat_n)]).wait()
        summed = inbox[group][0].astype(jnp.float32)
        for n in range(1, feat_n):
            summed = summed + inbox[group][n].astype(jnp.float32)
        full[group][me_s, me_f] = summed.astype(full[group].dtype)
        for n in range(1, feat_n * (samp_n if group else 1)):
            copy = pltpu.make_async_remote_copy(
                full[group].at[me_s, me_f], full[group].at[me_s, me_f],
                ag_send.at[group, n], ag_recv.at[group, me_s, me_f],
                device_id={
                    "feat": wrap(me_f + n % feat_n, feat_n), "samp": wrap(me_s + n // feat_n, samp_n)
                },
            )
            copy.start()
            gather.append(copy)

    def pass_on(group):
        for k in range(1, feat_n):
            source = wrap(me_f + k, feat_n)
            landed = full[group].at[me_s, source]
            pltpu.make_async_copy(landed, landed, ag_recv.at[group, me_s, source]).wait()
        for k in range(1, samp_n):
            copy = pltpu.make_async_remote_copy(
                full[group].at[me_s], full[group].at[me_s],
                fw_send.at[group, k - 1], fw_recv.at[group, me_s],
                device_id={"samp": wrap(me_s + k, samp_n)},
            )
            copy.start()
            forward.append(copy)

    def cross_arrived():
        for n in range(1, feat_n * samp_n):
            from_f, from_s = wrap(me_f + n % feat_n, feat_n), wrap(me_s + n // feat_n, samp_n)
            landed = full[1].at[from_s, from_f]
            pltpu.make_async_copy(landed, landed, ag_recv.at[1, from_s, from_f]).wait()

    def arrived(group):
        for k in range(1, samp_n):
            source = wrap(me_s + k, samp_n)
            landed = full[group].at[source]
            pltpu.make_async_copy(landed, landed, fw_recv.at[group, source]).wait()

    groups = range(len(part))
    for group in groups:
        sum_and_gather(group)
    pass_on(0)
    arrived(0)

    def put(p, q, value):
        high = value.astype(jnp.bfloat16)
        low = (value - high.astype(jnp.float32)).astype(jnp.bfloat16)
        ghl[p, pl.ds(0, rows), pl.ds(q * rows, rows)] = high
        ghl[p, pl.ds(rows, rows), pl.ds(q * rows, rows)] = low

    gain = []
    for p in every:
        block = full[0][p].reshape(feat_n * slab_a, rows)[:rows]
        put(p, p, block)
        norm = jnp.sum(jnp.where(row_id == col_id, block, 0.0), axis=0, keepdims=True) + 1.0
        gain.append(lam_total / norm)
    if pairs:
        cross_arrived()
        cross_sum = full[1][0].astype(jnp.float32)
        for s in range(1, samp_n):
            cross_sum = cross_sum + full[1][s].astype(jnp.float32)
        cross_sum = cross_sum.reshape(feat_n * slab_b, rows)
        for n, (p, q) in enumerate(pairs):
            block = cross_sum[n * rows : (n + 1) * rows]
            put(p, q, block)
            put(q, p, block.T)

    def apply(p, change):
        return jnp.dot(
            jnp.concatenate([change, change], axis=1), ghl[p], preferred_element_type=jnp.float32
        ) * (1.0 / lam_total)

    base = None
    for p in every:
        term = apply(p, (alpha[p] * signs[p]).astype(jnp.bfloat16))
        base = term if base is None else base + term
    for r in range(ROUNDS):
        local = list(alpha)
        coupled = [None] * samp_n
        moved = None
        for b in range(rows // BLOCK):
            for p in every:
                margins = base[:, p * rows : (p + 1) * rows]
                if coupled[p] is not None:
                    margins = margins + coupled[p]
                updated = jnp.clip(local[p] + gain[p] * (1.0 - signs[p] * margins), 0.0, 1.0)
                updated = jnp.where(place[r][p] == float(b), updated, local[p])
                change = ((updated - local[p]) * signs[p]).astype(jnp.bfloat16)
                local[p] = updated
                term = apply(p, change)
                mine = term[:, p * rows : (p + 1) * rows]
                coupled[p] = mine if coupled[p] is None else coupled[p] + mine
                moved = term if moved is None else moved + term
        base = base + moved * (1.0 / samp_n)
        alpha = [alpha[p] + (local[p] - alpha[p]) * (1.0 / samp_n) for p in every]

    alpha_mine, score_mine = alpha[0], base[:, :rows]
    for p in range(1, samp_n):
        alpha_mine = jnp.where(me_s == p, alpha[p], alpha_mine)
        score_mine = jnp.where(me_s == p, base[:, p * rows : (p + 1) * rows], score_mine)
    alpha_out[...] = alpha_mine
    score_out[...] = score_mine

    for copy in exchange + scatter + gather + forward:
        copy.wait_send()


def per_device(features, labels, alpha_start, order):
    rows, depth = features.shape
    label_n = labels.shape[1]
    labels, alpha_start = labels.T, alpha_start.T
    feat_n, samp_n = lax.axis_size("feat"), lax.axis_size("samp")
    width = depth // samp_n
    piece = width // PIECES
    pair_n = samp_n * (samp_n - 1) // 2
    sizes = [round_up(-(-rows // feat_n), 8)]
    if pair_n:
        sizes.append(round_up(-(-pair_n * rows // feat_n), 8))
    lam_total = REG_SCALE * depth * feat_n
    dma = pltpu.SemaphoreType.DMA
    others, peers = max(samp_n - 1, 1), max(feat_n - 1, 1)
    alpha, scores = pl.pallas_call(
        functools.partial(kernel, feat_n, samp_n, lam_total),
        out_shape=[jax.ShapeDtypeStruct((label_n, rows), jnp.float32)] * 2,
        in_specs=[pl.BlockSpec(memory_space=pltpu.HBM)] * 4,
        out_specs=[pl.BlockSpec(memory_space=pltpu.VMEM)] * 2,
        scratch_shapes=[
            pltpu.VMEM((others, PIECES, rows, piece), features.dtype),
            pltpu.VMEM((samp_n, PIECES, rows, piece), features.dtype),
            pltpu.VMEM((samp_n,) + labels.shape, labels.dtype),
            pltpu.VMEM((samp_n,) + alpha_start.shape, jnp.float32),
            pltpu.VMEM((samp_n,) + order.shape, order.dtype),
            [pltpu.VMEM((feat_n, size, rows), kind) for size, kind in zip(sizes, KINDS)],
            [pltpu.VMEM((feat_n, size, rows), kind) for size, kind in zip(sizes, KINDS)],
            [pltpu.VMEM((samp_n, feat_n, size, rows), kind) for size, kind in zip(sizes, KINDS)],
            pltpu.VMEM((samp_n, 2 * rows, samp_n * rows), jnp.bfloat16),
            pltpu.SemaphoreType.REGULAR,
            pltpu.SemaphoreType.REGULAR,
            pltpu.SemaphoreType.REGULAR,
            dma((samp_n * PIECES + 3,)),
            dma((others, PIECES)),
            dma((samp_n, PIECES)),
            dma((others, 3)),
            dma((samp_n, 3)),
            dma((2, peers)),
            dma((2, feat_n)),
            dma((2, samp_n * feat_n)),
            dma((2, samp_n, feat_n)),
            dma((2, others)),
            dma((2, samp_n)),
        ],
        compiler_params=pltpu.CompilerParams(
            collective_id=0, has_side_effects=True, vmem_limit_bytes=56000000
        ),
    )(*(pltpu.with_memory_space_constraint(x, pltpu.HBM) for x in (features, labels, alpha_start, order)))
    return alpha.T, scores.T


def solution(mesh):
    return jax.shard_map(
        per_device,
        mesh=mesh,
        in_specs=(P("samp", "feat"), P("samp", None), P("samp", None), P(None, "samp")),
        out_specs=(P("samp", None), P("samp", None)),
        check_vma=False,
    )
```
